32 devices in a mesh: cohort: 2 (over y), bx: 16 (over z, x, core).
Axes of the slice: x: 2, y: 2, z: 4, core: 2. Of those that a mesh axis runs over, the one named last changes fastest.
Arguments:
- bold: bfloat16 [256, 12, 4096], P('cohort', None, 'bx'), parts along dimension 0, may hold values from -6 to 6
- nbr_table: int32 [256, 4096], P('cohort', 'bx'), parts along dimension 0, may hold values from -1 to 767, as said below
- subject: int32 [256], P('cohort'), parts along dimension 0, may hold values from 0 to 7
Outputs:
- spread: float32 [8192], P(('cohort', 'bx')), parts along dimension 0
- gram_mean: float32 [256, 128], P('cohort'), parts along dimension 0
The draws below stay inside these ranges and needn't reach their ends.
There are 2 independent parts, one for each index of `cohort`. The reference program is written for one: setup_inputs(seed, part) draws one part's arguments, and reference() takes and returns one part's arrays. A program takes and returns all parts, laid end to end along the dimension named above; each array names one. Nothing has to cross between parts.
Inputs may be any that keep to these rules, and one draw needn't show every extreme that they name: `nbr_table`: rows 125 to 127 are all -1 and row (124) // 2 names the centre itself (256 + its place in its block). Any other entry is -1 or the place, in the window made of the previous block, the centre's own block and the next block (768 voxels in order), of a voxel at most 147 voxels away from the centre in voxel order; no entry names a voxel outside the cohort's 4096 voxels.
All inputs are finite; a program needn't handle non-finite values.
Results may differ from the reference program's by a relative error of at most 0.0003.
Values may be sent and summed in bfloat16 or wider, within the bound.
No kernel may reach another device: no remote copies, remote signals or barrier semaphores. Data moves between devices by JAX's collectives and lax.ppermute only.
A program may use at most 64 MiB of HBM per device.

```python
import jax
import jax.numpy as jnp
from jax import lax

VB = 256
E = 128
TP = 12
NB = 125
NBP = 128
SUBJ = 8
ROW = 8
PLANE = 64
NVOX = 4096
N_BX = 16


def draw_nbr_table(key, part):
    member = jnp.arange(NB, dtype=jnp.int32)
    along_x = member // 25 - 2
    along_y = member // 5 % 5 - 2
    along_z = member % 5 - 2
    base_offset = along_x * PLANE + along_y * ROW + along_z
    is_centre = (member == (NB - 1) // 2)[:, None]
    subkeys = jax.random.split(key, 2)
    jitter = jax.random.randint(subkeys[0], (NB, NVOX), -1, 2).astype(jnp.int32)
    jitter = jnp.where(is_centre, 0, jitter)
    keeping = jax.random.randint(subkeys[1], (NB, NVOX), 0, 4) > 0
    keeping = keeping | is_centre
    centre_ids = jnp.arange(NVOX, dtype=jnp.int32)[None, :]
    target = centre_ids + base_offset[:, None] + jitter
    inside = keeping & (target >= 0) & (target < NVOX)
    local_place = target - (centre_ids // VB - 1) * VB
    table = jnp.where(inside, local_place, -1).astype(jnp.int32)
    padding = jnp.full((NBP - NB, NVOX), -1, jnp.int32)
    return jnp.concatenate([table, padding], axis=0)


def plant(array, rng, least, top_value):
    shape = array.shape
    index_at = [jax.random.randint(jax.random.fold_in(rng, axis), (), 0, shape[axis]) for axis in range(len(shape))]
    array = array.at[tuple(index_at)].set(least)
    longest = shape.index(max(shape))
    index_at[longest] = (index_at[longest] + 1) % shape[longest]
    return array.at[tuple(index_at)].set(top_value)


def levels(rng, extent, cuts, low, top_value):
    gain = 1.0
    for dim, shards_of in cuts:
        heights = jax.random.uniform(jax.random.fold_in(jax.random.fold_in(rng, 6), dim), (shards_of,), jnp.float32, low / len(cuts), top_value / len(cuts))
        gain = gain * jnp.repeat(jnp.exp(heights), extent[dim] // shards_of).reshape((-1,) + (1,) * (len(extent) - 1 - dim))
    return gain


def normal_values(rng, dims, scale, limit, shards=(), held_as=jnp.bfloat16):
    values = jax.random.normal(rng, dims, jnp.float32) * scale
    if len(shards) > 0:
        values = levels(rng, dims, shards, -0.22, 0.18) * values
    return jnp.clip(values, min=-limit, max=limit).astype(held_as)


def setup_inputs(seed: int = 0, part: int = 0) -> dict:
    key_list = jax.random.split(jax.random.key(seed), 4)
    part_keys = jax.random.split(jax.random.fold_in(key_list[3], part), 4)
    bold = normal_values(part_keys[0], (E, TP, NVOX), 1.0, 6.0, ((2, 16),))
    nbr_table = draw_nbr_table(jax.random.fold_in(jax.random.fold_in(key_list[3], part), 71), part)
    subject = plant(jax.random.randint(part_keys[2], (E,), 0, SUBJ), jax.random.fold_in(part_keys[2], 1), 0, SUBJ - 1).astype(jnp.int32)
    return dict(bold=bold, nbr_table=nbr_table, subject=subject)


VARIANCE_FLOOR = 0.05

def normalize(series):
    values = series.astype(jnp.float32)
    centred = values - lax.optimization_barrier(jnp.mean(values, axis=1, keepdims=True))
    divisor = jnp.sqrt(lax.optimization_barrier(jnp.sum(centred * centred, axis=1, keepdims=True)) + 1.0)
    return (centred / divisor).astype(jnp.bfloat16)

def zscore(correl, onehot, counts):
    averages = jnp.einsum('es,ecj->scj', onehot, correl, precision=lax.Precision.HIGHEST) / counts[:, None, None]
    expanded = jnp.einsum('es,scj->ecj', onehot, averages, precision=lax.Precision.HIGHEST)
    deviation = correl - expanded
    variance = jnp.einsum('es,ecj->scj', onehot, deviation * deviation, precision=lax.Precision.HIGHEST) / counts[:, None, None]
    divisor = jnp.einsum('es,scj->ecj', onehot, jnp.sqrt(variance + VARIANCE_FLOOR), precision=lax.Precision.HIGHEST)
    return deviation / divisor

def reference(bold, nbr_table, subject):
    normed = normalize(bold).astype(jnp.float32)
    onehot = (subject[:, None] == jnp.arange(SUBJ, dtype=jnp.int32)[None, :]).astype(jnp.float32)
    counts = jnp.maximum(lax.optimization_barrier(jnp.sum(onehot, axis=0)), 1.0)
    padded = jnp.pad(normed, ((0, 0), (0, 0), (VB, VB)))

    def one_block(block_id):
        first_col = (block_id * VB).astype(jnp.int32)
        lookup = lax.dynamic_slice_in_dim(nbr_table, first_col, VB, 1)
        usable = (lookup >= 0).T
        position = (jnp.where(lookup >= 0, lookup, 0) + first_col).T.reshape(-1).astype(jnp.int32)
        centre = lax.dynamic_slice_in_dim(normed, first_col, VB, 2)
        gathered = jnp.take(padded, position, axis=2).reshape(E, TP, VB, NBP)
        correl = jnp.einsum('etc,etcj->ecj', centre, gathered, precision=lax.Precision.HIGHEST)
        correl = jnp.where(usable[None], correl, jnp.float32(0.0))
        features = zscore(correl, onehot, counts)
        kernel = jnp.einsum('ecj,fcj->cef', features, features, precision=lax.Precision.HIGHEST) / NB
        return (lax.optimization_barrier(jnp.sum(kernel, axis=0)), jnp.sqrt(lax.optimization_barrier(jnp.sum(kernel * kernel, axis=(1, 2))) / E))
    block_sums, spreads = lax.map(one_block, jnp.arange(N_BX).astype(jnp.int32))
    return (spreads.reshape(-1), lax.optimization_barrier(jnp.sum(block_sums, axis=0)) / NVOX)
```

```python
import functools

import jax
import jax.numpy as jnp
from jax import lax
from jax.experimental import pallas as pl
from jax.experimental.pallas import tpu as pltpu
from jax.sharding import PartitionSpec as P

NB = 125
VARIANCE_FLOOR = 0.05
REACH = 147
LANES = 128
GROUP = 64
WINDOW = 384
HALO = (WINDOW - GROUP) // 2
TPAD = 16
ECHUNK = 16


def normalize(series):
    values = series.astype(jnp.float32)
    centred = values - jnp.mean(values, axis=1, keepdims=True)
    divisor = jnp.sqrt(jnp.sum(centred * centred, axis=1, keepdims=True) + 1.0)
    return (centred / divisor).astype(jnp.bfloat16)


def body(sub_col, sub_row, nt, idx, win, spread, gram, lhs, prod, sums):
    epochs = sub_col.shape[0]
    depth = ECHUNK * TPAD
    group_id = pl.program_id(0)
    groups = pl.num_programs(0)
    first = pl.multiple_of(group_id * GROUP, GROUP)
    parity = group_id % 2
    lane0 = pl.multiple_of((group_id // 2) * LANES, LANES)

    @pl.when(group_id == 0)
    def _():
        gram[...] = jnp.zeros_like(gram)

    row_e = lax.broadcasted_iota(jnp.int32, (ECHUNK, depth), 0)
    col_e = lax.broadcasted_iota(jnp.int32, (ECHUNK, depth), 1) // TPAD
    diagonal = row_e == col_e

    def chunk(k, carry):
        at = pl.multiple_of(k * depth, depth)
        for c in range(GROUP):
            row = nt[pl.ds(first + c, 1), pl.ds(at, depth)]
            block = jnp.where(diagonal, jnp.broadcast_to(row, (ECHUNK, depth)), 0.0)
            lhs[c * ECHUNK : (c + 1) * ECHUNK, :] = block.astype(jnp.bfloat16)
        out = jnp.dot(
            lhs[...],
            win[parity, pl.ds(at, depth), pl.ds(lane0, WINDOW)],
            preferred_element_type=jnp.float32,
        )
        to = pl.multiple_of(k * ECHUNK, ECHUNK)
        prod[:, pl.ds(to, ECHUNK), :] = out.reshape(GROUP, ECHUNK, WINDOW)
        return carry

    lax.fori_loop(0, epochs // ECHUNK, chunk, 0)

    same = sub_col[...] == sub_row[...]
    same_f = same.astype(jnp.float32)
    counts = jnp.maximum(jnp.sum(same_f, axis=1, keepdims=True), 1.0)
    inverse = jnp.broadcast_to(1.0 / counts, (epochs, LANES))
    same_b = same_f.astype(jnp.bfloat16)
    same_2 = jnp.concatenate([same_b, same_b], axis=1)

    def select(c):
        place = jnp.broadcast_to(idx[pl.ds(first + c, 1), :], (epochs, LANES))
        low = place & (LANES - 1)
        high = place >> 7
        out = jnp.zeros((epochs, LANES), jnp.float32)
        for tile in range(WINDOW // LANES):
            part = prod[c, :, tile * LANES : (tile + 1) * LANES]
            taken = jnp.take_along_axis(part, low, axis=1, mode="promise_in_bounds")
            out = jnp.where(high == tile, taken, out)
        return out

    def pair(p, carry):
        cs = (2 * p, 2 * p + 1)
        x = jnp.concatenate([select(c) for c in cs], axis=1)
        hi = x.astype(jnp.bfloat16)
        lo = (x - hi.astype(jnp.float32)).astype(jnp.bfloat16)
        inv = jnp.concatenate([inverse, inverse], axis=1)
        mean = jnp.dot(same_2, jnp.concatenate([hi, lo], axis=0), preferred_element_type=jnp.float32) * inv
        dev = x - mean
        var = jnp.dot(same_b, (dev * dev).astype(jnp.bfloat16), preferred_element_type=jnp.float32) * inv
        feat = (dev * lax.rsqrt(var + VARIANCE_FLOOR)).astype(jnp.bfloat16)
        total = None
        for i, c in enumerate(cs):
            f = feat[:, i * LANES : (i + 1) * LANES]
            kern = lax.dot_general(f, f, (((1,), (1,)), ((), ())), preferred_element_type=jnp.float32)
            sums[pl.ds(first + c, 1), :] = jnp.sum(kern * kern, axis=0, keepdims=True)
            total = kern if total is None else total + kern
        gram[...] += total
        return carry

    lax.fori_loop(0, GROUP // 2, pair, 0, unroll=2)

    @pl.when(group_id == groups - 1)
    def _():
        ones = jnp.ones((8, epochs), jnp.float32)
        rows = lax.dot_general(
            ones, sums[...], (((1,), (1,)), ((), ())),
            precision=lax.Precision.HIGHEST, preferred_element_type=jnp.float32,
        )
        spread[...] = jnp.sqrt(rows[:1] * (1.0 / (NB * NB)) / epochs)


def per_device(bold, nbr_table, subject):
    epochs, points, block_len = bold.shape
    count = lax.axis_size("bx")
    ends = count - 1
    head = bold[:, :, :HALO]
    tail = bold[:, :, block_len - HALO :]
    before = lax.ppermute(tail, "bx", [(i, i + 1) for i in range(ends)])
    after = lax.ppermute(head, "bx", [(i + 1, i) for i in range(ends)])
    own = normalize(bold)
    padt = ((0, 0), (0, TPAD - points), (0, 0))
    rows = epochs * TPAD
    nt = jnp.pad(own, padt).reshape(rows, block_len).T.astype(jnp.float32)
    ext = jnp.concatenate([normalize(before), own, normalize(after)], axis=2)
    ext = jnp.pad(ext, padt).reshape(rows, block_len + 2 * HALO)
    width = block_len + 2 * HALO - GROUP
    win = jnp.stack([ext[:, :width], ext[:, GROUP:]])
    centre_group = jnp.arange(block_len, dtype=jnp.int32) // GROUP * GROUP
    start = block_len - HALO + centre_group
    idx = jnp.where(nbr_table >= 0, nbr_table - start[None, :], -1).T
    groups = block_len // GROUP
    slots = nbr_table.shape[0]
    whole = lambda *shape: pl.BlockSpec(shape, lambda g: (0,) * len(shape))
    spread, totals = pl.pallas_call(
        body,
        grid=(groups,),
        in_specs=[
            whole(epochs, 1),
            whole(1, epochs),
            whole(block_len, rows),
            whole(block_len, slots),
            whole(2, rows, width),
        ],
        out_specs=[whole(1, block_len), whole(epochs, epochs)],
        out_shape=[
            jax.ShapeDtypeStruct((1, block_len), jnp.float32),
            jax.ShapeDtypeStruct((epochs, epochs), jnp.float32),
        ],
        scratch_shapes=[
            pltpu.VMEM((GROUP * ECHUNK, ECHUNK * TPAD), jnp.bfloat16),
            pltpu.VMEM((GROUP, epochs, WINDOW), jnp.float32),
            pltpu.VMEM((block_len, epochs), jnp.float32),
        ],
        compiler_params=pltpu.CompilerParams(
            dimension_semantics=("arbitrary",), vmem_limit_bytes=56 * 1024 * 1024
        ),
        name="searchlight",
    )(subject[:, None], subject[None, :], nt, idx, win)
    gram_mean = lax.psum(totals, "bx") / (NB * block_len * count)
    return (spread.reshape(-1), gram_mean)


def solution(mesh):
    return jax.shard_map(
        per_device,
        mesh=mesh,
        in_specs=(P("cohort", None, "bx"), P("cohort", "bx"), P("cohort")),
        out_specs=(P(("cohort", "bx")), P("cohort", None)),
        check_vma=False,
    )
```

```python
import functools

import jax
import jax.numpy as jnp
from jax import lax
from jax.experimental import pallas as pl
from jax.experimental.pallas import tpu as pltpu
from jax.sharding import PartitionSpec as P

NB = 125
VARIANCE_FLOOR = 0.05
REACH = 147
LANES = 128
GROUP = 64
WINDOW = 384
HALO = (WINDOW - GROUP) // 2
TPAD = 16
ECHUNK = 16


def normalize(series):
    values = series.astype(jnp.float32)
    centred = values - jnp.mean(values, axis=1, keepdims=True)
    divisor = jnp.sqrt(jnp.sum(centred * centred, axis=1, keepdims=True) + 1.0)
    return (centred / divisor).astype(jnp.bfloat16)


def body(sub_col, sub_row, nt, idx, win_even, win_odd, spread, gram, lhs, prod, sums, win, xs, devs, feats):
    epochs = sub_col.shape[0]
    depth = ECHUNK * TPAD
    group_id = pl.program_id(0)
    groups = pl.num_programs(0)
    first = pl.multiple_of(group_id * GROUP, GROUP)
    parity = group_id % 2
    lane0 = pl.multiple_of((group_id // 2) * LANES, LANES)

    @pl.when(group_id == 0)
    def _():
        gram[...] = jnp.zeros_like(gram)

    @pl.when(parity == 0)
    def _():
        win[...] = win_even[:, pl.ds(lane0, WINDOW)]

    @pl.when(parity == 1)
    def _():
        win[...] = win_odd[:, pl.ds(lane0, WINDOW)]

    row_e = lax.broadcasted_iota(jnp.int32, (ECHUNK, depth), 0)
    col_e = lax.broadcasted_iota(jnp.int32, (ECHUNK, depth), 1) // TPAD
    diagonal = row_e == col_e

    def chunk(k, carry):
        at = pl.multiple_of(k * depth, depth)
        for c in range(GROUP):
            row = nt[pl.ds(first + c, 1), pl.ds(at, depth)]
            block = jnp.where(diagonal, jnp.broadcast_to(row, (ECHUNK, depth)), 0.0)
            lhs[c * ECHUNK : (c + 1) * ECHUNK, :] = block.astype(jnp.bfloat16)
        out = jnp.dot(lhs[...], win[pl.ds(at, depth), :], preferred_element_type=jnp.float32)
        to = pl.multiple_of(k * ECHUNK, ECHUNK)
        prod[:, pl.ds(to, ECHUNK), :] = out.reshape(GROUP, ECHUNK, WINDOW)
        return carry

    lax.fori_loop(0, epochs // ECHUNK, chunk, 0)

    same = sub_col[...] == sub_row[...]
    same_f = same.astype(jnp.float32)
    counts = jnp.maximum(jnp.sum(same_f, axis=1, keepdims=True), 1.0)
    inverse = jnp.broadcast_to(1.0 / counts, (epochs, 2 * LANES))
    same_b = same_f.astype(jnp.bfloat16)
    same_2 = jnp.concatenate([same_b, same_b], axis=1)

    def select(c):
        place = jnp.broadcast_to(idx[pl.ds(first + c, 1), :], (epochs, LANES))
        low = place & (LANES - 1)
        high = place >> 7
        out = jnp.zeros((epochs, LANES), jnp.float32)
        for tile in range(WINDOW // LANES):
            part = prod[c, :, tile * LANES : (tile + 1) * LANES]
            taken = jnp.take_along_axis(part, low, axis=1, mode="promise_in_bounds")
            out = jnp.where(high == tile, taken, out)
        return out

    xs[...] = jnp.zeros_like(xs)
    devs[...] = jnp.zeros_like(devs)
    feats[...] = jnp.zeros_like(feats)
    pairs = GROUP // 2

    def step(p, carry):
        done = first + 2 * jnp.maximum(p - 3, 0)
        total = None
        for i in range(2):
            f = feats[:, i * LANES : (i + 1) * LANES]
            kern = lax.dot_general(f, f, (((1,), (1,)), ((), ())), preferred_element_type=jnp.float32)
            sums[pl.ds(done + i, 1), :] = jnp.sum(kern * kern, axis=0, keepdims=True)
            total = kern if total is None else total + kern
        dev = devs[...]
        var = jnp.dot(same_b, (dev * dev).astype(jnp.bfloat16), preferred_element_type=jnp.float32) * inverse
        x = xs[...]
        hi = x.astype(jnp.bfloat16)
        lo = (x - hi.astype(jnp.float32)).astype(jnp.bfloat16)
        mean = jnp.dot(same_2, jnp.concatenate([hi, lo], axis=0), preferred_element_type=jnp.float32) * inverse
        gram[...] += total
        feats[...] = (dev * lax.rsqrt(var + VARIANCE_FLOOR)).astype(jnp.bfloat16)
        devs[...] = x - mean
        nxt = 2 * jnp.minimum(p, pairs - 1)
        for i in range(2):
            xs[:, i * LANES : (i + 1) * LANES] = select(nxt + i)
        return carry

    lax.fori_loop(0, pairs + 3, step, 0)

    @pl.when(group_id == groups - 1)
    def _():
        ones = jnp.ones((8, epochs), jnp.float32)
        rows = lax.dot_general(
            ones, sums[...], (((1,), (1,)), ((), ())),
            precision=lax.Precision.HIGHEST, preferred_element_type=jnp.float32,
        )
        spread[...] = jnp.sqrt(rows[:1] * (1.0 / (NB * NB)) / epochs)


def total_over(values, axis):
    count = lax.axis_size(axis)
    if count & (count - 1):
        return lax.psum(values, axis)
    step = 1
    while step < count:
        values = values + lax.ppermute(values, axis, [(i, i ^ step) for i in range(count)])
        step *= 2
    return values


def per_device(bold, nbr_table, subject):
    epochs, points, block_len = bold.shape
    count = lax.axis_size("bx")
    ends = count - 1
    rows = epochs * TPAD
    own = jnp.pad(normalize(bold), ((0, 0), (0, TPAD - points), (0, 0))).reshape(rows, block_len)
    before = lax.ppermute(own[:, block_len - HALO :], "bx", [(i, i + 1) for i in range(ends)])
    after = lax.ppermute(own[:, :HALO], "bx", [(i + 1, i) for i in range(ends)])
    nt = own.T.astype(jnp.float32)
    width = block_len + 2 * HALO - GROUP
    win_even = jnp.concatenate([before, own, after[:, : HALO - GROUP]], axis=1)
    win_odd = jnp.concatenate([before[:, GROUP:], own, after], axis=1)
    centre_group = jnp.arange(block_len, dtype=jnp.int32) // GROUP * GROUP
    start = block_len - HALO + centre_group
    idx = jnp.where(nbr_table >= 0, nbr_table - start[None, :], -1).T
    groups = block_len // GROUP
    slots = nbr_table.shape[0]
    whole = lambda *shape: pl.BlockSpec(shape, lambda g: (0,) * len(shape))
    spread, totals = pl.pallas_call(
        body,
        grid=(groups,),
        in_specs=[
            whole(epochs, 1),
            whole(1, epochs),
            whole(block_len, rows),
            whole(block_len, slots),
            whole(rows, width),
            whole(rows, width),
        ],
        out_specs=[whole(1, block_len), whole(epochs, epochs)],
        out_shape=[
            jax.ShapeDtypeStruct((1, block_len), jnp.float32),
            jax.ShapeDtypeStruct((epochs, epochs), jnp.float32),
        ],
        scratch_shapes=[
            pltpu.VMEM((GROUP * ECHUNK, ECHUNK * TPAD), jnp.bfloat16),
            pltpu.VMEM((GROUP, epochs, WINDOW), jnp.float32),
            pltpu.VMEM((block_len, epochs), jnp.float32),
            pltpu.VMEM((rows, WINDOW), jnp.bfloat16),
            pltpu.VMEM((epochs, 2 * LANES), jnp.float32),
            pltpu.VMEM((epochs, 2 * LANES), jnp.float32),
            pltpu.VMEM((epochs, 2 * LANES), jnp.bfloat16),
        ],
        compiler_params=pltpu.CompilerParams(
            dimension_semantics=("arbitrary",), vmem_limit_bytes=56 * 1024 * 1024
        ),
        name="searchlight",
    )(subject[:, None], subject[None, :], nt, idx, win_even, win_odd)
    gram_mean = total_over(totals, "bx") / (NB * block_len * count)
    return (spread.reshape(-1), gram_mean)


def solution(mesh):
    return jax.shard_map(
        per_device,
        mesh=mesh,
        in_specs=(P("cohort", None, "bx"), P("cohort", "bx"), P("cohort")),
        out_specs=(P(("cohort", "bx")), P("cohort", None)),
        check_vma=False,
    )
```

```python
import functools

import jax
import jax.numpy as jnp
from jax import lax
from jax.experimental import pallas as pl
from jax.experimental.pallas import tpu as pltpu
from jax.sharding import PartitionSpec as P

NB = 125
VARIANCE_FLOOR = 0.05
REACH = 147
LANES = 128
GROUP = 64
WINDOW = 384
HALO = (WINDOW - GROUP) // 2
TPAD = 16
ECHUNK = 16
BATCH = 8


def normalize(series):
    values = series.astype(jnp.float32)
    centred = values - jnp.mean(values, axis=1, keepdims=True)
    divisor = jnp.sqrt(jnp.sum(centred * centred, axis=1, keepdims=True) + 1.0)
    return (centred / divisor).astype(jnp.bfloat16)


def body(sub_col, sub_row, nt, idx, before, own, after, spread, gram, lhs, prod, sums, win, xs, devs, feats):
    epochs = sub_col.shape[0]
    depth = ECHUNK * TPAD
    group_id = pl.program_id(0)
    groups = pl.num_programs(0)
    first = pl.multiple_of(group_id * GROUP, GROUP)

    @pl.when(group_id == 0)
    def _():
        gram[...] = jnp.zeros_like(gram)
        xs[...] = jnp.zeros_like(xs)
        devs[...] = jnp.zeros_like(devs)
        feats[...] = jnp.zeros_like(feats)

    for shift in range(0, own.shape[1], GROUP):

        @pl.when(group_id == shift // GROUP)
        def _(shift=shift):
            def fill(r, carry):
                at = pl.ds(pl.multiple_of(r * depth, depth), depth)
                parts = []
                left = HALO - shift
                if left > 0:
                    parts.append(before[at, shift:])
                low = max(-left, 0)
                high = min(own.shape[1], WINDOW - left)
                parts.append(own[at, low:high])
                rest = WINDOW - left - high
                if rest > 0:
                    parts.append(after[at, :rest])
                win[at, :] = jnp.concatenate(parts, axis=1)
                return carry

            lax.fori_loop(0, own.shape[0] // depth, fill, 0)

    row_e = lax.broadcasted_iota(jnp.int32, (ECHUNK, depth), 0)
    col_e = lax.broadcasted_iota(jnp.int32, (ECHUNK, depth), 1) // TPAD
    diagonal = row_e == col_e

    def chunk(k, carry):
        at = pl.multiple_of(k * depth, depth)
        for c in range(GROUP):
            row = nt[pl.ds(first + c, 1), pl.ds(at, depth)]
            block = jnp.where(diagonal, jnp.broadcast_to(row, (ECHUNK, depth)), 0.0)
            lhs[c * ECHUNK : (c + 1) * ECHUNK, :] = block.astype(jnp.bfloat16)
        out = jnp.dot(lhs[...], win[pl.ds(at, depth), :], preferred_element_type=jnp.float32)
        to = pl.multiple_of(k * ECHUNK, ECHUNK)
        prod[:, pl.ds(to, ECHUNK), :] = out.reshape(GROUP, ECHUNK, WINDOW)
        return carry

    lax.fori_loop(0, epochs // ECHUNK, chunk, 0)

    same = sub_col[...] == sub_row[...]
    same_f = same.astype(jnp.float32)
    counts = jnp.maximum(jnp.sum(same_f, axis=1, keepdims=True), 1.0)
    inverse = jnp.broadcast_to(1.0 / counts, (epochs, BATCH * LANES))
    same_b = same_f.astype(jnp.bfloat16)
    same_2 = jnp.concatenate([same_b, same_b], axis=1)

    def select(c):
        place = jnp.broadcast_to(idx[pl.ds(first + c, 1), :], (epochs, LANES))
        low = place & (LANES - 1)
        high = place >> 7
        out = jnp.zeros((epochs, LANES), jnp.float32)
        for tile in range(WINDOW // LANES):
            part = prod[c, :, tile * LANES : (tile + 1) * LANES]
            taken = jnp.take_along_axis(part, low, axis=1, mode="promise_in_bounds")
            out = jnp.where(high == tile, taken, out)
        return out

    batches = GROUP // BATCH

    def step(p, carry):
        done = BATCH * jnp.maximum(group_id * batches + p - 3, 0)
        total = None
        for i in range(BATCH):
            f = feats[:, i * LANES : (i + 1) * LANES]
            kern = lax.dot_general(f, f, (((1,), (1,)), ((), ())), preferred_element_type=jnp.float32)
            sums[pl.ds(done + i, 1), :] = jnp.sum(kern * kern, axis=0, keepdims=True)
            total = kern if total is None else total + kern
        dev = devs[...]
        var = jnp.dot(same_b, (dev * dev).astype(jnp.bfloat16), preferred_element_type=jnp.float32) * inverse
        x = xs[...]
        hi = x.astype(jnp.bfloat16)
        lo = (x - hi.astype(jnp.float32)).astype(jnp.bfloat16)
        mean = jnp.dot(same_2, jnp.concatenate([hi, lo], axis=0), preferred_element_type=jnp.float32) * inverse
        gram[...] += total
        feats[...] = (dev * lax.rsqrt(var + VARIANCE_FLOOR)).astype(jnp.bfloat16)
        devs[...] = x - mean
        nxt = BATCH * jnp.minimum(p, batches - 1)
        for i in range(BATCH):
            xs[:, i * LANES : (i + 1) * LANES] = select(nxt + i)
        return carry

    drain = jnp.where(group_id == groups - 1, 3, 0)
    lax.fori_loop(0, batches + drain, step, 0)

    @pl.when(group_id == groups - 1)
    def _():
        ones = jnp.ones((8, epochs), jnp.float32)
        rows = lax.dot_general(
            ones, sums[...], (((1,), (1,)), ((), ())),
            precision=lax.Precision.HIGHEST, preferred_element_type=jnp.float32,
        )
        spread[...] = jnp.sqrt(rows[:1] * (1.0 / (NB * NB)) / epochs)


def total_over(values, axis):
    count = lax.axis_size(axis)
    if count & (count - 1):
        return lax.psum(values, axis)
    step = 1
    while step < count:
        values = values + lax.ppermute(values, axis, [(i, i ^ step) for i in range(count)])
        step *= 2
    return values


def per_device(bold, nbr_table, subject):
    epochs, points, block_len = bold.shape
    count = lax.axis_size("bx")
    ends = count - 1
    rows = epochs * TPAD
    own = jnp.pad(normalize(bold), ((0, 0), (0, TPAD - points), (0, 0))).reshape(rows, block_len)
    before = lax.ppermute(own[:, block_len - HALO :], "bx", [(i, i + 1) for i in range(ends)])
    after = lax.ppermute(own[:, :HALO], "bx", [(i + 1, i) for i in range(ends)])
    nt = own.T.astype(jnp.float32)
    centre_group = jnp.arange(block_len, dtype=jnp.int32) // GROUP * GROUP
    start = block_len - HALO + centre_group
    idx = jnp.where(nbr_table >= 0, nbr_table - start[None, :], -1).T
    groups = block_len // GROUP
    slots = nbr_table.shape[0]
    whole = lambda *shape: pl.BlockSpec(shape, lambda g: (0,) * len(shape))
    spread, totals = pl.pallas_call(
        body,
        grid=(groups,),
        in_specs=[
            whole(epochs, 1),
            whole(1, epochs),
            whole(block_len, rows),
            whole(block_len, slots),
            whole(rows, HALO),
            whole(rows, block_len),
            whole(rows, HALO),
        ],
        out_specs=[whole(1, block_len), whole(epochs, epochs)],
        out_shape=[
            jax.ShapeDtypeStruct((1, block_len), jnp.float32),
            jax.ShapeDtypeStruct((epochs, epochs), jnp.float32),
        ],
        scratch_shapes=[
            pltpu.VMEM((GROUP * ECHUNK, ECHUNK * TPAD), jnp.bfloat16),
            pltpu.VMEM((GROUP, epochs, WINDOW), jnp.float32),
            pltpu.VMEM((block_len, epochs), jnp.float32),
            pltpu.VMEM((rows, WINDOW), jnp.bfloat16),
            pltpu.VMEM((epochs, BATCH * LANES), jnp.float32),
            pltpu.VMEM((epochs, BATCH * LANES), jnp.float32),
            pltpu.VMEM((epochs, BATCH * LANES), jnp.bfloat16),
        ],
        compiler_params=pltpu.CompilerParams(
            dimension_semantics=("arbitrary",), vmem_limit_bytes=56 * 1024 * 1024
        ),
        name="searchlight",
    )(subject[:, None], subject[None, :], nt, idx, before, own, after)
    gram_mean = total_over(totals, "bx") / (NB * block_len * count)
    return (spread.reshape(-1), gram_mean)


def solution(mesh):
    return jax.shard_map(
        per_device,
        mesh=mesh,
        in_specs=(P("cohort", None, "bx"), P("cohort", "bx"), P("cohort")),
        out_specs=(P(("cohort", "bx")), P("cohort", None)),
        check_vma=False,
    )
```
